32 devices in a mesh: gx: 8 (over z, y), gy: 4 (over x, core).
Axes of the slice: x: 2, y: 2, z: 4, core: 2. Of those that a mesh axis runs over, the one named last changes fastest.
Arguments:
- basis: bfloat16 [40960, 120], P(('gx', 'gy')), may hold values from -0.03125 to 0.03125
- snapshots: bfloat16 [40960, 256], P(('gx', 'gy')), may hold values from -6 to 6
- derivatives: bfloat16 [40960, 256], P(('gx', 'gy')), may hold values from -24 to 24
- quad_pairs: int32 [2, 7260], replicated, may hold values from 0 to 119, as said below
- penalty: float32 [7381], replicated, may hold values from 0.5 to 8
Outputs:
- operator: float32 [120, 7381], replicated
The draws below stay inside these ranges and needn't reach their ends.
Inputs may be any that keep to these rules, and one draw needn't show every extreme that they name: `quad_pairs`: every pair (i, j) with 0 <= i <= j < 120 stands in exactly one column, in an order drawn from the seed.
All inputs are finite; a program needn't handle non-finite values.
Results may differ from the reference program's by a relative error of at most 0.0003.
Values sent between devices are 32-bit elements; how exact they have to be, the bound alone decides.
No kernel may reach another device: no remote copies, remote signals or barrier semaphores. Data moves between devices by JAX's collectives and lax.ppermute only.
A program may use at most 64 MiB of HBM per device.

```python
import math
import jax
import jax.numpy as jnp
from jax import lax

R = 120
NQ = 7260
F = 7381
SNAPS = 256
ITERS = 2
NDOF = 40960


def draw_quad_pairs(key, part):
    first, second = jnp.triu_indices(R)
    order = jax.random.permutation(key, first.shape[0])
    return jnp.stack([first[order], second[order]]).astype(jnp.int32)


def block_scale(own_key, extent, cuts, smallest, largest):
    loudness = 1.0
    for axis_at, shards_of in cuts:
        draws = jax.random.uniform(jax.random.fold_in(jax.random.fold_in(own_key, 6), axis_at), (shards_of,), jnp.float32, smallest / len(cuts), largest / len(cuts))
        loudness = loudness * jnp.repeat(jnp.exp(draws), extent[axis_at] // shards_of).reshape((-1,) + (1,) * (len(extent) - 1 - axis_at))
    return loudness


def noise(key, shape, spread, most, pieces=(), kind=jnp.bfloat16):
    entries = spread * jax.random.normal(key, shape, jnp.float32)
    if pieces:
        entries = entries * block_scale(key, shape, pieces, -0.22, 0.18)
    return jnp.clip(entries, -most, most).astype(kind)


def setup_inputs(seed: int = 0) -> dict:
    splits = jax.random.split(jax.random.key(seed), 6)
    basis = noise(splits[0], (NDOF, R), NDOF ** -0.5, 0.03125, ((0, 32),))
    snapshots = noise(splits[1], (NDOF, SNAPS), 1.0, 6.0, ((0, 32),))
    derivatives = noise(splits[2], (NDOF, SNAPS), 4.0, 24.0, ((0, 32),))
    quad_pairs = draw_quad_pairs(jax.random.fold_in(splits[5], 71), 0)
    penalty = jnp.clip(jnp.exp(jax.random.uniform(splits[4], (F,), jnp.float32, math.log(0.5), math.log(8.0))), 0.5, 8.0)
    return {"basis": basis, "snapshots": snapshots, "derivatives": derivatives, "quad_pairs": quad_pairs, "penalty": penalty}


def feature_rows(index, coeffs, pairs):
    total = coeffs.shape[0]
    count = pairs.shape[1]
    linear = coeffs[jnp.clip(index - 1, 0, total - 1)]
    slot = jnp.clip(index - 1 - total, 0, count - 1)
    quad = coeffs[pairs[0, slot]] * coeffs[pairs[1, slot]]
    column = index[:, None]
    width = 1 + total + count
    return jnp.where(column == 0, jnp.float32(1.0), jnp.where(column <= total, linear, jnp.where(column < width, quad, jnp.float32(0.0)))).astype(jnp.float32)

def reference(basis, snapshots, derivatives, quad_pairs, penalty):
    dims = (((0,), (0,)), ((), ()))
    coeffs = lax.dot_general(basis, snapshots, dims, preferred_element_type=jnp.float32)
    rates = lax.dot_general(basis, derivatives, dims, preferred_element_type=jnp.float32)
    width = 1 + R + NQ
    data = feature_rows(jnp.arange(width, dtype=jnp.int32), coeffs, quad_pairs)
    snaps = snapshots.shape[1]
    inner = (((1,), (1,)), ((), ()))
    normal = lax.dot_general(data, data, inner, precision=lax.Precision.HIGHEST, preferred_element_type=jnp.float32) / snaps
    normal = normal + jnp.diag(penalty)
    target = lax.dot_general(data, rates, inner, precision=lax.Precision.HIGHEST, preferred_element_type=jnp.float32) / math.sqrt(snaps)
    solution = jnp.zeros_like(target)
    residual = target
    direction = target
    norm_now = lax.optimization_barrier(jnp.sum(residual * residual, axis=0))
    for step in range(ITERS):
        image = jnp.dot(normal, direction, precision=lax.Precision.HIGHEST, preferred_element_type=jnp.float32)
        alpha = norm_now / lax.optimization_barrier(jnp.sum(direction * image, axis=0))
        solution = solution + alpha * direction
        residual = residual - alpha * image
        norm_next = lax.optimization_barrier(jnp.sum(residual * residual, axis=0))
        direction = residual + norm_next / norm_now * direction
        norm_now = norm_next
    return solution.T
```

```python
import math

import jax
import jax.numpy as jnp
from jax import lax
from jax.experimental import pallas as pl
from jax.experimental.pallas import tpu as pltpu
from jax.sharding import PartitionSpec as P

LANES = 128
TILE = 256
HIGHEST = lax.Precision.HIGHEST
F32 = jnp.float32
BF16 = jnp.bfloat16


def round_up(value, unit):
    return -(-value // unit) * unit


def dot(a, b, contract, precision=None):
    return lax.dot_general(
        a, b, (contract, ((), ())), precision=precision, preferred_element_type=F32
    )


def split(value):
    high = value.astype(BF16)
    return high, (value - high.astype(F32)).astype(BF16)


def project(basis_ref, snaps_ref, rates_ref, out_ref):
    order = basis_ref.shape[1]
    basis = basis_ref[...]
    out_ref[...] = jnp.zeros_like(out_ref)
    out_ref[0, :order, :] = dot(basis, snaps_ref[...], ((0,), (0,)))
    out_ref[1, :order, :] = dot(basis, rates_ref[...], ((0,), (0,)))


def pick(table, index):
    return jnp.take_along_axis(table, index, axis=1, mode="promise_in_bounds")


def fit(order, width, sums_ref, index_ref, weight_ref, out_ref, table_ref, left_ref, b_ref, s_ref, v_ref, acc_ref):
    snaps = sums_ref.shape[2]
    padded = index_ref.shape[1]
    tiles = padded // TILE
    lane = lax.broadcasted_iota(jnp.int32, (snaps, LANES), 1)
    linear = jnp.where(lane < order, jnp.transpose(sums_ref[0]), 0.0)
    table_ref[...] = jnp.where(lane == order, 1.0, linear)
    cross = dot(linear, linear, ((1,), (1,)), HIGHEST)
    squares = linear * linear
    gram = 1.0 + cross + 0.5 * (cross * cross + dot(squares, squares, ((1,), (1,)), HIGHEST))
    rates = sums_ref[1, :order, :] * (1.0 / math.sqrt(snaps))
    u = dot(rates, gram, ((1,), (0,)), HIGHEST)
    m0 = jnp.sum(rates * u, axis=1, keepdims=True)
    shift = jnp.sum(u * u, axis=1, keepdims=True) / (snaps * m0)
    along = u * (1.0 / snaps) - shift * rates
    mean = jnp.sum(weight_ref[...], axis=1, keepdims=True) * (1.0 / width)
    high, low = split(rates)
    left_ref[0:order, :] = high
    left_ref[2 * order : 3 * order, :] = low
    high, low = split(along)
    left_ref[order : 2 * order, :] = high
    left_ref[3 * order : 4 * order, :] = low
    v_ref[...] = jnp.zeros_like(v_ref)
    acc_ref[...] = jnp.zeros_like(acc_ref)

    def tile(step, carry):
        base = pl.multiple_of(step * TILE, TILE)
        table = table_ref[...]
        parts = []
        for half in range(TILE // LANES):
            place = pl.ds(pl.multiple_of(base + half * LANES, LANES), LANES)
            first = jnp.broadcast_to(index_ref[0:1, place], table.shape)
            second = jnp.broadcast_to(index_ref[1:2, place], table.shape)
            parts.append(pick(table, first) * pick(table, second))
        data = jnp.concatenate(parts, axis=1)
        data_high, data_low = split(data)
        one = dot(left_ref[...], data_high, ((1,), (0,)))
        two = dot(left_ref[0 : 2 * order, :], data_low, ((1,), (0,)))
        both = one[: 2 * order] + one[2 * order :] + two
        place = pl.ds(base, TILE)
        b = both[:order]
        extra = weight_ref[0:1, place] - mean
        scaled = extra * b
        s = both[order:] + scaled
        b_ref[:, place] = b
        s_ref[:, place] = s
        v_ref[...] += dot(scaled.astype(BF16), data_high, ((1,), (1,)))
        acc_ref[0] += scaled * b
        acc_ref[1] += s * s
        acc_ref[2] += extra * s * s
        acc_ref[3] += scaled * s
        return carry

    lax.fori_loop(0, tiles, tile, 0)
    total = [jnp.sum(acc_ref[k], axis=1, keepdims=True) for k in range(4)]
    bb_extra, ss, ss_extra, bs_extra = total
    ratio = bb_extra / m0
    alpha0 = 1.0 / (shift + mean + ratio)
    perp = ss - ratio * bb_extra
    image = dot(along, gram, ((1,), (0,)), HIGHEST) + v_ref[...] - ratio * u
    energy = (
        jnp.sum(image * image, axis=1, keepdims=True) * (1.0 / snaps)
        + mean * perp
        + ss_extra
        - 2.0 * ratio * bs_extra
        + ratio * ratio * bb_extra
    )
    rr1 = alpha0 * alpha0 * perp
    beta = rr1 / m0
    alpha1 = rr1 / (alpha0 * alpha0 * energy - rr1 * beta / alpha0)
    on_b = alpha0 + alpha1 * (beta + alpha0 * ratio)
    on_s = -alpha1 * alpha0

    def combine(step, carry):
        place = pl.ds(pl.multiple_of(step * TILE, TILE), TILE)
        out_ref[:, place] = on_b * b_ref[:, place] + on_s * s_ref[:, place]
        return carry

    whole = width // TILE
    lax.fori_loop(0, whole, combine, 0)
    if whole * TILE < width:
        rest = slice(whole * TILE, width)
        out_ref[:, rest] = on_b * b_ref[:, rest] + on_s * s_ref[:, rest]


def on_device(basis, snapshots, derivatives, quad_pairs, penalty):
    axes = ("gx", "gy")
    devices = lax.axis_size("gx") * lax.axis_size("gy")
    order = basis.shape[1]
    snaps = snapshots.shape[1]
    count = quad_pairs.shape[1]
    width = 1 + order + count
    padded = round_up(width, TILE)
    assert order + 2 <= LANES
    part = pl.pallas_call(
        project,
        out_shape=jax.ShapeDtypeStruct((2, LANES, snaps), F32),
        name="project",
    )(basis, snapshots, derivatives)
    rows = 2 * LANES
    full = round_up(rows, devices)
    pieces = jnp.pad(part.reshape(rows, snaps), ((0, full - rows), (0, 0)))
    pieces = pieces.reshape(devices, full // devices, snaps)
    pieces = lax.all_to_all(pieces, axes, 0, 0, tiled=True)
    summed = jnp.sum(pieces, axis=0, keepdims=True)
    spread = jnp.broadcast_to(summed, pieces.shape)
    whole = lax.all_to_all(spread, axes, 0, 0, tiled=True)
    sums = whole.reshape(full, snaps)[:rows].reshape(2, LANES, snaps)
    counting = jnp.arange(order, dtype=jnp.int32)
    ones = jnp.full((1 + order,), order, jnp.int32)
    blank = jnp.full((2, padded - width), order + 1, jnp.int32)
    head = jnp.stack([jnp.concatenate([ones[:1], counting]), ones])
    index = jnp.concatenate([head, quad_pairs, blank], axis=1)
    weight = jnp.pad(penalty, (0, padded - width)).reshape(1, padded)
    return pl.pallas_call(
        lambda *refs: fit(order, width, *refs),
        out_shape=jax.ShapeDtypeStruct((order, width), F32),
        scratch_shapes=[
            pltpu.VMEM((snaps, LANES), F32),
            pltpu.VMEM((4 * order, snaps), BF16),
            pltpu.VMEM((order, padded), F32),
            pltpu.VMEM((order, padded), F32),
            pltpu.VMEM((order, snaps), F32),
            pltpu.VMEM((4, order, TILE), F32),
        ],
        compiler_params=pltpu.CompilerParams(vmem_limit_bytes=48 * 2**20),
        name="fit",
    )(sums, index, weight)


def solution(mesh):
    split_rows = P(("gx", "gy"), None)
    return jax.shard_map(
        on_device,
        mesh=mesh,
        in_specs=(split_rows, split_rows, split_rows, P(), P()),
        out_specs=P(),
        check_vma=False,
    )
```

```python
import math

import jax
import jax.numpy as jnp
from jax import lax
from jax.experimental import pallas as pl
from jax.experimental.pallas import tpu as pltpu
from jax.sharding import PartitionSpec as P

LANES = 128
TILE = 256
F32 = jnp.float32
BF16 = jnp.bfloat16
ROWS = ((1,), (0,))


def limit(mebibytes):
    return pltpu.CompilerParams(vmem_limit_bytes=mebibytes * 2**20)


def round_up(value, unit):
    return -(-value // unit) * unit


def dot(a, b, contract=ROWS):
    return lax.dot_general(a, b, (contract, ((), ())), preferred_element_type=F32)


def split(value):
    high = value.astype(BF16)
    return high, (value - high.astype(F32)).astype(BF16)


def project(basis_ref, snaps_ref, rates_ref, out_ref, basis_buf, snaps_buf, rates_buf, sems):
    order = basis_ref.shape[0]
    count, size = sems.shape[0], snaps_buf.shape[0] // sems.shape[0]
    copies = []
    for k in range(count):
        here = pl.ds(k * size, size)
        mine = [
            pltpu.make_async_copy(basis_ref.at[:, here], basis_buf.at[:, here], sems.at[k, 0]),
            pltpu.make_async_copy(snaps_ref.at[here, :], snaps_buf.at[here, :], sems.at[k, 1]),
            pltpu.make_async_copy(rates_ref.at[here, :], rates_buf.at[here, :], sems.at[k, 2]),
        ]
        for copy in mine:
            copy.start()
        copies.append(mine)
    total = [0.0, 0.0]
    for k in range(count):
        for copy in copies[k]:
            copy.wait()
        here = slice(k * size, (k + 1) * size)
        basis = basis_buf[:, here]
        total = [t + dot(basis, buf[here, :]) for t, buf in zip(total, (snaps_buf, rates_buf))]
    for k in range(2):
        out_ref[k, :order, :] = total[k]
        out_ref[k, order:, :] = jnp.zeros((LANES - order, out_ref.shape[2]), F32)


def add_up(parts_ref, out_ref):
    out_ref[...] = jnp.broadcast_to(jnp.sum(parts_ref[...], axis=0, keepdims=True), out_ref.shape)


def fit(
    sums_ref, index_ref, weight_ref, out_ref,
    table_ref, left_ref, gram_ref, high_ref, low_ref, b_ref, s_ref, v_ref, acc_ref, extra_ref, mix_ref, x_ref, sems,
):
    order, width = out_ref.shape
    snaps = sums_ref.shape[2]
    padded = index_ref.shape[1]
    pairs = padded // (2 * TILE)
    spare = padded // TILE - 2 * pairs

    def place(start, size):
        return pl.ds(start if isinstance(start, int) else pl.multiple_of(start, TILE), size)

    def build(start):
        here = place(start, TILE)
        row = lax.broadcasted_iota(jnp.int32, (LANES, TILE), 0)
        factors = []
        for k in range(2):
            hot = jnp.where(row == index_ref[k : k + 1, here], 1.0, 0.0).astype(BF16)
            factors.append(dot(table_ref[...], jnp.concatenate([hot, hot], axis=0)))
        high, low = split(factors[0] * factors[1])
        high_ref[:, here] = high
        low_ref[:, here] = low

    def multiply(start):
        here = place(start, TILE)
        one = dot(left_ref[...], high_ref[:, here])
        two = dot(left_ref[0 : 2 * order, :], low_ref[:, here])
        both = one[: 2 * order] + one[2 * order :] + two
        b = both[:order]
        b_ref[:, here] = b
        s_ref[:, here] = both[order:] + extra_ref[0:1, here] * b

    def gather(start, size):
        here = place(start, size)
        b = b_ref[:, here]
        s = s_ref[:, here]
        extra = extra_ref[0:1, here]
        scaled = extra * b
        v_ref[...] += dot(scaled.astype(BF16), high_ref[:, here], ((1,), (1,)))
        square = s * s
        for k, term in enumerate((scaled * b, square, extra * square, scaled * s)):
            acc_ref[k] += sum(term[:, i : i + LANES] for i in range(0, size, LANES))

    def on_pair(stage, index):
        for half in range(2):
            stage((2 * index + half) * TILE)

    coeffs = sums_ref[0]
    coeffs_high, coeffs_low = split(coeffs)
    high, low = split(jnp.transpose(coeffs))
    lane = lax.broadcasted_iota(jnp.int32, (snaps, LANES), 1)
    table_ref[:, :LANES] = jnp.where(lane == order, 1.0, high.astype(F32)).astype(BF16)
    table_ref[:, LANES:] = low
    mean = jnp.sum(weight_ref[...], axis=1, keepdims=True) * (1.0 / width)
    extra_ref[...] = weight_ref[...] - mean
    v_ref[...] = jnp.zeros_like(v_ref)
    acc_ref[...] = jnp.zeros_like(acc_ref)
    on_pair(build, 0)
    on_pair(build, 1)
    if spare:
        build(2 * pairs * TILE)
    table = table_ref[...]
    cross = dot(table, jnp.concatenate([coeffs_high, coeffs_high], axis=0)) + dot(high, coeffs_low)
    square = coeffs * coeffs
    square_high, square_low = split(square)
    turned_high, turned_low = split(jnp.transpose(square))
    squares = dot(
        jnp.concatenate([turned_high, turned_low], axis=1),
        jnp.concatenate([square_high, square_high], axis=0),
    ) + dot(turned_high, square_low)
    gram_high, gram_low = split(1.0 + cross + 0.5 * (cross * cross + squares))
    gram_ref[0] = gram_high
    gram_ref[1] = gram_low

    def times_gram(high, low):
        both = dot(jnp.concatenate([high, low], axis=0), gram_ref[0])
        return both[:order] + both[order:] + dot(high, gram_ref[1])

    rates = sums_ref[1, :order, :] * (1.0 / math.sqrt(snaps))
    rates_high, rates_low = split(rates)
    u = times_gram(rates_high, rates_low)
    m0 = jnp.sum(rates * u, axis=1, keepdims=True)
    shift = jnp.sum(u * u, axis=1, keepdims=True) / (snaps * m0)
    along = u * (1.0 / snaps) - shift * rates
    along_high, along_low = split(along)
    left_ref[0:order, :] = rates_high
    left_ref[order : 2 * order, :] = along_high
    left_ref[2 * order : 3 * order, :] = rates_low
    left_ref[3 * order : 4 * order, :] = along_low
    on_pair(multiply, 0)
    if spare:
        multiply(2 * pairs * TILE)

    def body(index, carry):
        gather((index - 1) * 2 * TILE, 2 * TILE)
        on_pair(multiply, index)
        on_pair(build, index + 1)
        return carry

    lax.fori_loop(1, pairs - 1, body, 0)
    gather((pairs - 2) * 2 * TILE, 2 * TILE)
    on_pair(multiply, pairs - 1)
    if spare:
        gather(2 * pairs * TILE, TILE)
    gather((pairs - 1) * 2 * TILE, 2 * TILE)

    total = [jnp.sum(acc_ref[k], axis=1, keepdims=True) for k in range(4)]
    bb_extra, ss, ss_extra, bs_extra = total
    ratio = bb_extra / m0
    alpha0 = 1.0 / (shift + mean + ratio)
    perp = ss - ratio * bb_extra
    image = times_gram(along_high, along_low) + v_ref[...] - ratio * u
    energy = (
        jnp.sum(image * image, axis=1, keepdims=True) * (1.0 / snaps)
        + mean * perp
        + ss_extra
        - 2.0 * ratio * bs_extra
        + ratio * ratio * bb_extra
    )
    rr1 = alpha0 * alpha0 * perp
    beta = rr1 / m0
    alpha1 = rr1 / (alpha0 * alpha0 * energy - rr1 * beta / alpha0)
    mix_ref[0] = jnp.broadcast_to(alpha0 + alpha1 * (beta + alpha0 * ratio), (order, LANES))
    mix_ref[1] = jnp.broadcast_to(-alpha1 * alpha0, (order, LANES))

    def copy(group):
        rows = pl.ds(pl.multiple_of(group * 8, 8), 8)
        return pltpu.make_async_copy(x_ref.at[rows, :], out_ref.at[rows, :], sems.at[group])

    def combine(group, carry):
        rows = pl.ds(pl.multiple_of(group * 8, 8), 8)
        on_b = mix_ref[0, rows, :]
        on_s = mix_ref[1, rows, :]
        for left in range(0, width, LANES):
            here = slice(left, min(left + LANES, width))
            size = here.stop - here.start
            x_ref[rows, here] = on_b[:, :size] * b_ref[rows, here] + on_s[:, :size] * s_ref[rows, here]
        copy(group).start()
        return carry

    def finish(group, carry):
        copy(group).wait()
        return carry

    lax.fori_loop(0, order // 8, combine, 0)
    lax.fori_loop(0, order // 8, finish, 0)


def on_device(basis, snapshots, derivatives, quad_pairs, penalty):
    axes = ("gx", "gy")
    devices = lax.axis_size("gx") * lax.axis_size("gy")
    length, order = basis.shape
    snaps = snapshots.shape[1]
    steps = length // TILE if length % TILE == 0 else 1
    count = quad_pairs.shape[1]
    width = 1 + order + count
    padded = round_up(width, TILE)
    assert order + 2 <= LANES and order % 8 == 0
    vmem = pl.BlockSpec(memory_space=pltpu.VMEM)
    part = pl.pallas_call(
        project,
        in_specs=(pl.BlockSpec(memory_space=pltpu.HBM),) * 3,
        out_shape=pltpu.VMEM((2, LANES, snaps), F32),
        out_specs=vmem,
        scratch_shapes=[
            pltpu.VMEM((order, length), BF16),
            pltpu.VMEM((length, snaps), BF16),
            pltpu.VMEM((length, snaps), BF16),
            pltpu.SemaphoreType.DMA((steps, 3)),
        ],
        compiler_params=limit(8),
        name="project",
    )(*(pltpu.with_memory_space_constraint(a, pltpu.HBM) for a in (basis.T, snapshots, derivatives)))
    rows = 2 * LANES
    full = round_up(rows, devices)
    pieces = jnp.pad(part.reshape(rows, snaps), ((0, full - rows), (0, 0)))
    pieces = pieces.reshape(devices, full // devices, snaps)
    pieces = lax.all_to_all(pieces, axes, 0, 0, tiled=True)
    spread = pl.pallas_call(
        add_up,
        out_shape=pltpu.VMEM(pieces.shape, F32),
        out_specs=vmem,
        compiler_params=limit(8),
        name="add_up",
    )(pieces)
    whole = lax.all_to_all(spread, axes, 0, 0, tiled=True)
    sums = whole.reshape(full, snaps)[:rows].reshape(2, LANES, snaps)
    counting = jnp.arange(order, dtype=jnp.int32)
    ones = jnp.full((1 + order,), order, jnp.int32)
    blank = jnp.full((2, padded - width), order + 1, jnp.int32)
    head = jnp.stack([jnp.concatenate([ones[:1], counting]), ones])
    index = jnp.concatenate([head, quad_pairs, blank], axis=1)
    weight = jnp.pad(penalty, (0, padded - width)).reshape(1, padded)
    return pl.pallas_call(
        fit,
        out_shape=jax.ShapeDtypeStruct((order, width), F32),
        in_specs=(vmem,) * 3,
        out_specs=pl.BlockSpec(memory_space=pl.ANY),
        scratch_shapes=[
            pltpu.VMEM((snaps, 2 * LANES), BF16),
            pltpu.VMEM((4 * order, snaps), BF16),
            pltpu.VMEM((2, snaps, snaps), BF16),
            pltpu.VMEM((snaps, padded), BF16),
            pltpu.VMEM((snaps, padded), BF16),
            pltpu.VMEM((order, padded), F32),
            pltpu.VMEM((order, padded), F32),
            pltpu.VMEM((order, snaps), F32),
            pltpu.VMEM((4, order, LANES), F32),
            pltpu.VMEM((1, padded), F32),
            pltpu.VMEM((2, order, LANES), F32),
            pltpu.VMEM((order, width), F32),
            pltpu.SemaphoreType.DMA((order // 8,)),
        ],
        compiler_params=limit(36),
        name="fit",
    )(sums, index, weight)


def solution(mesh):
    split_rows = P(("gx", "gy"), None)
    return jax.shard_map(
        on_device,
        mesh=mesh,
        in_specs=(split_rows, split_rows, split_rows, P(), P()),
        out_specs=P(),
        check_vma=False,
    )
```

```python
import math

import jax
import jax.numpy as jnp
from jax import lax
from jax.experimental import pallas as pl
from jax.experimental.pallas import tpu as pltpu
from jax.sharding import PartitionSpec as P

LANES = 128
TILE = 256
F32 = jnp.float32
BF16 = jnp.bfloat16
ROWS = ((1,), (0,))


def limit(mebibytes):
    return pltpu.CompilerParams(vmem_limit_bytes=mebibytes * 2**20)


def round_up(value, unit):
    return -(-value // unit) * unit


def dot(a, b, contract=ROWS):
    return lax.dot_general(a, b, (contract, ((), ())), preferred_element_type=F32)


def split(value):
    high = value.astype(BF16)
    return high, (value - high.astype(F32)).astype(BF16)


def project(core_ref, basis_ref, snaps_ref, rates_ref, mine_ref, other_ref, basis_buf, snaps_buf, rates_buf, sems):
    order = basis_ref.shape[0]
    count, size = sems.shape[0], snaps_buf.shape[0] // sems.shape[0]
    copies = []
    for k in range(count):
        here = pl.ds(k * size, size)
        mine = [
            pltpu.make_async_copy(basis_ref.at[:, here], basis_buf.at[:, here], sems.at[k, 0]),
            pltpu.make_async_copy(snaps_ref.at[here, :], snaps_buf.at[here, :], sems.at[k, 1]),
            pltpu.make_async_copy(rates_ref.at[here, :], rates_buf.at[here, :], sems.at[k, 2]),
        ]
        for copy in mine:
            copy.start()
        copies.append(mine)
    total = [0.0, 0.0]
    for k in range(count):
        for copy in copies[k]:
            copy.wait()
        here = slice(k * size, (k + 1) * size)
        basis = basis_buf[:, here]
        total = [t + dot(basis, buf[here, :]) for t, buf in zip(total, (snaps_buf, rates_buf))]
    blank = jnp.zeros((LANES - order, mine_ref.shape[2]), F32)
    first = core_ref[0] == 0
    for k in range(2):
        left, right = jnp.split(total[k], 2, axis=1)
        mine_ref[k, :order, :] = jnp.where(first, left, right)
        other_ref[k, :order, :] = jnp.where(first, right, left)
        mine_ref[k, order:, :] = blank
        other_ref[k, order:, :] = blank


def add_up(parts_ref, out_ref):
    devices = parts_ref.shape[0]
    for kind in range(2):
        total = parts_ref[kind]
        for k in range(kind + 2, devices, 2):
            total += parts_ref[k]
        for k in range(kind, devices, 2):
            out_ref[k] = total


def one_hot(index_ref, k, here):
    row = lax.broadcasted_iota(jnp.int32, (LANES, TILE), 0)
    return jnp.where(row == index_ref[k : k + 1, here], 1.0, 0.0).astype(BF16)


def fit(
    core_ref, mine_ref, other_ref, index_ref, weight_ref, out_ref,
    table_ref, left_ref, gram_ref, even_ref, odd_ref, rest_ref, b_ref, s_ref, v_ref, acc_ref, extra_ref, mix_ref, x_ref, sems,
):
    order, width = out_ref.shape
    snaps = 2 * mine_ref.shape[2]
    padded = index_ref.shape[1]
    pairs = padded // (4 * TILE) * 2
    spare = padded // TILE - 2 * pairs

    def place(start, size):
        return pl.ds(start if isinstance(start, int) else pl.multiple_of(start, TILE), size)

    def build(data_ref, start, size):
        for left in range(0, size, TILE):
            here = place(start + left, TILE)
            factors = []
            for k in range(2):
                hot = one_hot(index_ref, k, here)
                factors.append(dot(table_ref[...], jnp.concatenate([hot, hot], axis=0)))
            high, low = split(factors[0] * factors[1])
            data_ref[0, :, left : left + TILE] = high
            data_ref[1, :, left : left + TILE] = low

    def multiply(data_ref, start, size):
        weighted = []
        terms = [0.0] * 4
        for left in range(0, size, TILE):
            here = place(start + left, TILE)
            high = data_ref[0, :, left : left + TILE]
            one = dot(left_ref[...], high)
            two = dot(left_ref[0 : 2 * order, :], data_ref[1, :, left : left + TILE])
            both = one[: 2 * order] + one[2 * order :] + two
            extra = extra_ref[0:1, here]
            b = both[:order]
            scaled = extra * b
            s = both[order:] + scaled
            b_ref[:, here] = b
            s_ref[:, here] = s
            weighted.append(scaled.astype(BF16))
            square = s * s
            new = (scaled * b, square, extra * square, scaled * s)
            terms = [t + n[:, :LANES] + n[:, LANES:] for t, n in zip(terms, new)]
        v_ref[...] += dot(jnp.concatenate(weighted, axis=1), data_ref[0], ((1,), (1,)))
        for k in range(4):
            acc_ref[k] += terms[k]

    def whole(k):
        mine, other = mine_ref[k], other_ref[k]
        first = core_ref[0] == 0
        return jnp.concatenate([jnp.where(first, mine, other), jnp.where(first, other, mine)], axis=1)

    coeffs = whole(0)
    coeffs_high, coeffs_low = split(coeffs)
    high, low = split(jnp.transpose(coeffs))
    lane = lax.broadcasted_iota(jnp.int32, (snaps, LANES), 1)
    table_ref[:, :LANES] = jnp.where(lane == order, 1.0, high.astype(F32)).astype(BF16)
    table_ref[:, LANES:] = low
    mean = jnp.sum(weight_ref[...], axis=1, keepdims=True) * (1.0 / width)
    extra_ref[...] = weight_ref[...] - mean
    v_ref[...] = jnp.zeros_like(v_ref)
    acc_ref[...] = jnp.zeros_like(acc_ref)
    wide = 2 * TILE
    build(even_ref, 0, wide)
    if spare:
        build(rest_ref, pairs * wide, spare * TILE)
    table = table_ref[...]
    cross = dot(table, jnp.concatenate([coeffs_high, coeffs_high], axis=0)) + dot(high, coeffs_low)
    square = coeffs * coeffs
    square_high, square_low = split(square)
    turned_high, turned_low = split(jnp.transpose(square))
    squares = dot(
        jnp.concatenate([turned_high, turned_low], axis=1),
        jnp.concatenate([square_high, square_high], axis=0),
    ) + dot(turned_high, square_low)
    gram_high, gram_low = split(1.0 + cross + 0.5 * (cross * cross + squares))
    gram_ref[0] = gram_high
    gram_ref[1] = gram_low

    def times_gram(high, low):
        both = dot(jnp.concatenate([high, low], axis=0), gram_ref[0])
        return both[:order] + both[order:] + dot(high, gram_ref[1])

    rates = whole(1)[:order] * (1.0 / math.sqrt(snaps))
    rates_high, rates_low = split(rates)
    u = times_gram(rates_high, rates_low)
    m0 = jnp.sum(rates * u, axis=1, keepdims=True)
    shift = jnp.sum(u * u, axis=1, keepdims=True) / (snaps * m0)
    along = u * (1.0 / snaps) - shift * rates
    along_high, along_low = split(along)
    left_ref[0:order, :] = rates_high
    left_ref[order : 2 * order, :] = along_high
    left_ref[2 * order : 3 * order, :] = rates_low
    left_ref[3 * order : 4 * order, :] = along_low
    if spare:
        multiply(rest_ref, pairs * wide, spare * TILE)

    def body(step, carry):
        first = 2 * step
        build(odd_ref, (first + 1) * wide, wide)
        multiply(even_ref, first * wide, wide)
        build(even_ref, (first + 2) * wide, wide)
        multiply(odd_ref, (first + 1) * wide, wide)
        return carry

    lax.fori_loop(0, pairs // 2 - 1, body, 0)
    build(odd_ref, (pairs - 1) * wide, wide)
    multiply(even_ref, (pairs - 2) * wide, wide)
    multiply(odd_ref, (pairs - 1) * wide, wide)

    total = [jnp.sum(acc_ref[k], axis=1, keepdims=True) for k in range(4)]
    bb_extra, ss, ss_extra, bs_extra = total
    ratio = bb_extra / m0
    alpha0 = 1.0 / (shift + mean + ratio)
    perp = ss - ratio * bb_extra
    image = times_gram(along_high, along_low) + v_ref[...] - ratio * u
    energy = (
        jnp.sum(image * image, axis=1, keepdims=True) * (1.0 / snaps)
        + mean * perp
        + ss_extra
        - 2.0 * ratio * bs_extra
        + ratio * ratio * bb_extra
    )
    rr1 = alpha0 * alpha0 * perp
    beta = rr1 / m0
    alpha1 = rr1 / (alpha0 * alpha0 * energy - rr1 * beta / alpha0)
    mix_ref[0] = jnp.broadcast_to(alpha0 + alpha1 * (beta + alpha0 * ratio), (order, LANES))
    mix_ref[1] = jnp.broadcast_to(-alpha1 * alpha0, (order, LANES))

    def copy(group):
        rows = pl.ds(pl.multiple_of(group * 8, 8), 8)
        return pltpu.make_async_copy(x_ref.at[rows, :], out_ref.at[rows, :], sems.at[group])

    def combine(group, carry):
        rows = pl.ds(pl.multiple_of(group * 8, 8), 8)
        on_b = mix_ref[0, rows, :]
        on_s = mix_ref[1, rows, :]
        for left in range(0, width, LANES):
            here = slice(left, min(left + LANES, width))
            size = here.stop - here.start
            x_ref[rows, here] = on_b[:, :size] * b_ref[rows, here] + on_s[:, :size] * s_ref[rows, here]
        copy(group).start()
        return carry

    def finish(group, carry):
        copy(group).wait()
        return carry

    lax.fori_loop(0, order // 8, combine, 0)
    lax.fori_loop(0, order // 8, finish, 0)


def on_device(basis, snapshots, derivatives, quad_pairs, penalty):
    axes = ("gx", "gy")
    devices = lax.axis_size("gx") * lax.axis_size("gy")
    length, order = basis.shape
    snaps = snapshots.shape[1]
    steps = length // TILE if length % TILE == 0 else 1
    count = quad_pairs.shape[1]
    width = 1 + order + count
    padded = round_up(width, TILE)
    assert order + 2 <= LANES and order % 8 == 0 and snaps % (2 * LANES) == 0
    assert lax.axis_size("gy") % 2 == 0
    vmem = pl.BlockSpec(memory_space=pltpu.VMEM)
    smem = pl.BlockSpec(memory_space=pltpu.SMEM)
    lanes = snaps // 2
    core = (lax.axis_index("gy") % 2).reshape(1)
    pair = [(k, k ^ 1) for k in range(lax.axis_size("gy"))]
    mine, other = pl.pallas_call(
        project,
        in_specs=(smem,) + (pl.BlockSpec(memory_space=pltpu.HBM),) * 3,
        out_shape=(pltpu.VMEM((2, LANES, lanes), F32),) * 2,
        out_specs=(vmem,) * 2,
        scratch_shapes=[
            pltpu.VMEM((order, length), BF16),
            pltpu.VMEM((length, snaps), BF16),
            pltpu.VMEM((length, snaps), BF16),
            pltpu.SemaphoreType.DMA((steps, 3)),
        ],
        compiler_params=limit(8),
        name="project",
    )(core, *(pltpu.with_memory_space_constraint(a, pltpu.HBM) for a in (basis.T, snapshots, derivatives)))
    mine = mine + lax.ppermute(other, "gy", pair)
    rows = 2 * LANES
    full = round_up(rows, devices)
    pieces = jnp.pad(mine.reshape(rows, lanes), ((0, full - rows), (0, 0)))
    pieces = pieces.reshape(devices, full // devices, lanes)
    pieces = lax.all_to_all(pieces, axes, 0, 0, tiled=True)
    spread = pl.pallas_call(
        add_up,
        out_shape=pltpu.VMEM(pieces.shape, F32),
        out_specs=vmem,
        compiler_params=limit(8),
        name="add_up",
    )(pieces)
    half = lax.all_to_all(spread, axes, 0, 0, tiled=True)
    half = half.reshape(full, lanes)[:rows].reshape(2, LANES, lanes)
    rest = lax.ppermute(half, "gy", pair)
    counting = jnp.arange(order, dtype=jnp.int32)
    ones = jnp.full((1 + order,), order, jnp.int32)
    blank = jnp.full((2, padded - width), order + 1, jnp.int32)
    head = jnp.stack([jnp.concatenate([ones[:1], counting]), ones])
    index = jnp.concatenate([head, quad_pairs, blank], axis=1)
    weight = jnp.pad(penalty, (0, padded - width)).reshape(1, padded)
    return pl.pallas_call(
        fit,
        out_shape=jax.ShapeDtypeStruct((order, width), F32),
        in_specs=(smem,) + (vmem,) * 4,
        out_specs=pl.BlockSpec(memory_space=pl.ANY),
        scratch_shapes=[
            pltpu.VMEM((snaps, 2 * LANES), BF16),
            pltpu.VMEM((4 * order, snaps), BF16),
            pltpu.VMEM((2, snaps, snaps), BF16),
            pltpu.VMEM((2, snaps, 2 * TILE), BF16),
            pltpu.VMEM((2, snaps, 2 * TILE), BF16),
            pltpu.VMEM((2, snaps, max(padded // TILE % 4, 1) * TILE), BF16),
            pltpu.VMEM((order, padded), F32),
            pltpu.VMEM((order, padded), F32),
            pltpu.VMEM((order, snaps), F32),
            pltpu.VMEM((4, order, LANES), F32),
            pltpu.VMEM((1, padded), F32),
            pltpu.VMEM((2, order, LANES), F32),
            pltpu.VMEM((order, width), F32),
            pltpu.SemaphoreType.DMA((order // 8,)),
        ],
        compiler_params=limit(36),
        name="fit",
    )(core, half, rest, index, weight)


def solution(mesh):
    split_rows = P(("gx", "gy"), None)
    return jax.shard_map(
        on_device,
        mesh=mesh,
        in_specs=(split_rows, split_rows, split_rows, P(), P()),
        out_specs=P(),
        check_vma=False,
    )
```

```python
import math

import jax
import jax.numpy as jnp
from jax import lax
from jax.experimental import pallas as pl
from jax.experimental.pallas import tpu as pltpu
from jax.sharding import PartitionSpec as P

LANES = 128
TILE = 256
F32 = jnp.float32
BF16 = jnp.bfloat16
ROWS = ((1,), (0,))


def limit(mebibytes):
    return pltpu.CompilerParams(vmem_limit_bytes=mebibytes * 2**20)


def round_up(value, unit):
    return -(-value // unit) * unit


def dot(a, b, contract=ROWS):
    return lax.dot_general(a, b, (contract, ((), ())), preferred_element_type=F32)


def split(value):
    high = value.astype(BF16)
    return high, (value - high.astype(F32)).astype(BF16)


def project(core_ref, basis_ref, snaps_ref, rates_ref, pairs_ref, mine_ref, other_ref, held_ref, basis_buf, snaps_buf, rates_buf, sems, pair_sem):
    order = basis_ref.shape[0]
    count, size = sems.shape[0], snaps_buf.shape[0] // sems.shape[0]
    copies = []
    for k in range(count):
        here = pl.ds(k * size, size)
        mine = [
            pltpu.make_async_copy(basis_ref.at[:, here], basis_buf.at[:, here], sems.at[k, 0]),
            pltpu.make_async_copy(snaps_ref.at[here, :], snaps_buf.at[here, :], sems.at[k, 1]),
            pltpu.make_async_copy(rates_ref.at[here, :], rates_buf.at[here, :], sems.at[k, 2]),
        ]
        for copy in mine:
            copy.start()
        copies.append(mine)
    hold = pltpu.make_async_copy(pairs_ref, held_ref, pair_sem)
    hold.start()
    total = [0.0, 0.0]
    for k in range(count):
        for copy in copies[k]:
            copy.wait()
        here = slice(k * size, (k + 1) * size)
        basis = basis_buf[:, here]
        total = [t + dot(basis, buf[here, :]) for t, buf in zip(total, (snaps_buf, rates_buf))]
    blank = jnp.zeros((LANES - order, mine_ref.shape[2]), F32)
    first = core_ref[0] == 0
    for k in range(2):
        left, right = jnp.split(total[k], 2, axis=1)
        mine_ref[k, :order, :] = jnp.where(first, left, right)
        other_ref[k, :order, :] = jnp.where(first, right, left)
        mine_ref[k, order:, :] = blank
        other_ref[k, order:, :] = blank
    hold.wait()


def add_up(parts_ref, out_ref):
    devices = parts_ref.shape[0]
    for kind in range(2):
        total = parts_ref[kind]
        for k in range(kind + 2, devices, 2):
            total += parts_ref[k]
        for k in range(kind, devices, 2):
            out_ref[k] = total


def one_hot(index):
    group = 16
    wanted = jnp.broadcast_to(index, (group, index.shape[1])).astype(BF16)
    row = lax.broadcasted_iota(jnp.int32, wanted.shape, 0).astype(F32)
    one, zero = jnp.ones(wanted.shape, BF16), jnp.zeros(wanted.shape, BF16)
    parts = [jnp.where((row + top).astype(BF16) == wanted, one, zero) for top in range(0, LANES, group)]
    return jnp.concatenate(parts, axis=0)


def product(table, hots):
    first, second = (dot(table, jnp.concatenate([hot, hot], axis=0)) for hot in hots)
    return split(first * second)


def make_table(coeffs, order):
    high, low = split(jnp.transpose(coeffs))
    lane = lax.broadcasted_iota(jnp.int32, high.shape, 1)
    high = jnp.where(lane == order, 1.0, high.astype(F32)).astype(BF16)
    return jnp.concatenate([high, low], axis=1)


def begin(order, width, mine_ref, pairs_ref, ready_ref, hot_ref, table_ref, index_ref):
    table_ref[...] = make_table(mine_ref[0], order)
    table = table_ref[...]
    padded = index_ref.shape[1]
    index_ref[0:2, : pairs_ref.shape[1]] = pairs_ref[...]
    turned = pltpu.roll(index_ref[...], order + 1, axis=1)
    row = lax.broadcasted_iota(jnp.int32, turned.shape, 0)
    lane = lax.broadcasted_iota(jnp.int32, turned.shape, 1)
    linear = jnp.where((row == 0) & (lane > 0), lane - 1, order)
    index_ref[...] = jnp.where(lane <= order, linear, jnp.where(lane < width, turned, order + 1))
    for left in range(0, padded, TILE):
        here = slice(left, left + TILE)
        index = index_ref[:, here].astype(F32)
        hots = [one_hot(index[k : k + 1]) for k in range(2)]
        for k in range(2):
            hot_ref[k, :, here] = hots[k]
        ready_ref[0, :, here], ready_ref[1, :, here] = product(table, hots)


def fit(
    core_ref, mine_ref, other_ref, ready_ref, hot_ref, own_ref, weight_ref, out_ref,
    far_ref, table_ref, left_ref, gram_ref, even_ref, odd_ref, rest_ref, b_ref, s_ref, v_ref, acc_ref, extra_ref, mix_ref, x_ref, sems,
):
    order, width = out_ref.shape
    lanes = mine_ref.shape[2]
    snaps = 2 * lanes
    padded = hot_ref.shape[2]
    pairs = padded // (4 * TILE) * 2
    spare = padded // TILE - 2 * pairs
    core = core_ref[0]

    def place(start, size):
        return pl.ds(start if isinstance(start, int) else pl.multiple_of(start, TILE), size)

    def build(data_ref, start, size):
        for left in range(0, size, TILE):
            here = place(start + left, TILE)
            there = slice(left, left + TILE)
            parts = product(far_ref[...], [hot_ref[k, :, here] for k in range(2)])
            for k in range(2):
                data_ref[k, core, :, there] = ready_ref[k, :, here]
                data_ref[k, 1 - core, :, there] = parts[k]

    def load(data_ref, k, left, size):
        return data_ref[k, :, :, left : left + size].reshape(snaps, size)

    def multiply(data_ref, start, size):
        weighted = []
        terms = [0.0] * 4
        for left in range(0, size, TILE):
            here = place(start + left, TILE)
            one = dot(left_ref[...], load(data_ref, 0, left, TILE))
            two = dot(left_ref[0 : 2 * order, :], load(data_ref, 1, left, TILE))
            both = one[: 2 * order] + one[2 * order :] + two
            extra = extra_ref[0:1, here]
            b = both[:order]
            scaled = extra * b
            s = both[order:] + scaled
            b_ref[:, here] = b
            s_ref[:, here] = s
            weighted.append(scaled.astype(BF16))
            square = s * s
            new = (scaled * b, square, extra * square, scaled * s)
            terms = [t + n[:, :LANES] + n[:, LANES:] for t, n in zip(terms, new)]
        v_ref[...] += dot(jnp.concatenate(weighted, axis=1), load(data_ref, 0, 0, size), ((1,), (1,)))
        for k in range(4):
            acc_ref[k] += terms[k]

    def whole(k):
        mine, other = mine_ref[k], other_ref[k]
        return jnp.concatenate([jnp.where(core == 0, mine, other), jnp.where(core == 0, other, mine)], axis=1)

    far_ref[...] = make_table(other_ref[0], order)
    table_ref[core] = own_ref[...]
    table_ref[1 - core] = far_ref[...]
    mean = jnp.sum(weight_ref[...], axis=1, keepdims=True) * (1.0 / width)
    extra_ref[...] = jnp.zeros_like(extra_ref)
    extra_ref[:, :width] = weight_ref[...] - mean
    v_ref[...] = jnp.zeros_like(v_ref)
    acc_ref[...] = jnp.zeros_like(acc_ref)
    wide = 2 * TILE
    build(even_ref, 0, wide)
    if spare:
        build(rest_ref, pairs * wide, spare * TILE)
    coeffs = whole(0)
    coeffs_high, coeffs_low = split(coeffs)
    table = table_ref[...].reshape(snaps, 2 * LANES)
    high, low = table[:, :LANES], table[:, LANES:]
    cross = dot(table, jnp.concatenate([coeffs_high, coeffs_high], axis=0)) + dot(high, coeffs_low)
    square_high, square_low = split(coeffs * coeffs)
    turned = high.astype(F32) + low.astype(F32)
    turned_high, turned_low = split(turned * turned)
    squares = dot(
        jnp.concatenate([turned_high, turned_low], axis=1),
        jnp.concatenate([square_high, square_high], axis=0),
    ) + dot(turned_high, square_low)
    gram_high, gram_low = split(1.0 + cross + 0.5 * (cross * cross + squares))
    gram_ref[0] = gram_high
    gram_ref[1] = gram_low

    def times_gram(high, low):
        both = dot(jnp.concatenate([high, low], axis=0), gram_ref[0])
        return both[:order] + both[order:] + dot(high, gram_ref[1])

    rates = whole(1)[:order] * (1.0 / math.sqrt(snaps))
    rates_high, rates_low = split(rates)
    u = times_gram(rates_high, rates_low)
    m0 = jnp.sum(rates * u, axis=1, keepdims=True)
    shift = jnp.sum(u * u, axis=1, keepdims=True) / (snaps * m0)
    along = u * (1.0 / snaps) - shift * rates
    along_high, along_low = split(along)
    left_ref[0:order, :] = rates_high
    left_ref[order : 2 * order, :] = along_high
    left_ref[2 * order : 3 * order, :] = rates_low
    left_ref[3 * order : 4 * order, :] = along_low
    if spare:
        multiply(rest_ref, pairs * wide, spare * TILE)

    def body(step, carry):
        first = 2 * step
        build(odd_ref, (first + 1) * wide, wide)
        multiply(even_ref, first * wide, wide)
        build(even_ref, (first + 2) * wide, wide)
        multiply(odd_ref, (first + 1) * wide, wide)
        return carry

    lax.fori_loop(0, pairs // 2 - 1, body, 0)
    build(odd_ref, (pairs - 1) * wide, wide)
    multiply(even_ref, (pairs - 2) * wide, wide)
    multiply(odd_ref, (pairs - 1) * wide, wide)

    total = [jnp.sum(acc_ref[k], axis=1, keepdims=True) for k in range(4)]
    bb_extra, ss, ss_extra, bs_extra = total
    ratio = bb_extra / m0
    alpha0 = 1.0 / (shift + mean + ratio)
    perp = ss - ratio * bb_extra
    image = times_gram(along_high, along_low) + v_ref[...] - ratio * u
    energy = (
        jnp.sum(image * image, axis=1, keepdims=True) * (1.0 / snaps)
        + mean * perp
        + ss_extra
        - 2.0 * ratio * bs_extra
        + ratio * ratio * bb_extra
    )
    rr1 = alpha0 * alpha0 * perp
    beta = rr1 / m0
    alpha1 = rr1 / (alpha0 * alpha0 * energy - rr1 * beta / alpha0)
    mix_ref[0] = jnp.broadcast_to(alpha0 + alpha1 * (beta + alpha0 * ratio), (order, LANES))
    mix_ref[1] = jnp.broadcast_to(-alpha1 * alpha0, (order, LANES))

    def copy(group):
        rows = pl.ds(pl.multiple_of(group * 8, 8), 8)
        return pltpu.make_async_copy(x_ref.at[rows, :], out_ref.at[rows, :], sems.at[group])

    def combine(group, carry):
        rows = pl.ds(pl.multiple_of(group * 8, 8), 8)
        on_b = mix_ref[0, rows, :]
        on_s = mix_ref[1, rows, :]
        for left in range(0, width, LANES):
            here = slice(left, min(left + LANES, width))
            size = here.stop - here.start
            x_ref[rows, here] = on_b[:, :size] * b_ref[rows, here] + on_s[:, :size] * s_ref[rows, here]
        copy(group).start()
        return carry

    def finish(group, carry):
        copy(group).wait()
        return carry

    lax.fori_loop(0, order // 8, combine, 0)
    lax.fori_loop(0, order // 8, finish, 0)


def on_device(basis, snapshots, derivatives, quad_pairs, penalty):
    axes = ("gx", "gy")
    devices = lax.axis_size("gx") * lax.axis_size("gy")
    length, order = basis.shape
    snaps = snapshots.shape[1]
    steps = length // TILE if length % TILE == 0 else 1
    count = quad_pairs.shape[1]
    width = 1 + order + count
    padded = round_up(width, TILE)
    assert order + 2 <= LANES and order % 8 == 0 and snaps % (2 * LANES) == 0
    assert lax.axis_size("gy") % 2 == 0
    vmem = pl.BlockSpec(memory_space=pltpu.VMEM)
    smem = pl.BlockSpec(memory_space=pltpu.SMEM)
    lanes = snaps // 2
    core = (lax.axis_index("gy") % 2).reshape(1)
    pair = [(k, k ^ 1) for k in range(lax.axis_size("gy"))]
    mine, other, held = pl.pallas_call(
        project,
        in_specs=(smem,) + (pl.BlockSpec(memory_space=pltpu.HBM),) * 4,
        out_shape=(pltpu.VMEM((2, LANES, lanes), F32),) * 2 + (pltpu.VMEM(quad_pairs.shape, jnp.int32),),
        out_specs=(vmem,) * 3,
        scratch_shapes=[
            pltpu.VMEM((order, length), BF16),
            pltpu.VMEM((length, snaps), BF16),
            pltpu.VMEM((length, snaps), BF16),
            pltpu.SemaphoreType.DMA((steps, 3)),
            pltpu.SemaphoreType.DMA,
        ],
        compiler_params=limit(8),
        name="project",
    )(core, *(pltpu.with_memory_space_constraint(a, pltpu.HBM) for a in (basis.T, snapshots, derivatives, quad_pairs)))
    mine, weight = lax.optimization_barrier((mine + lax.ppermute(other, "gy", pair), penalty.reshape(1, width)))
    rows = 2 * LANES
    full = round_up(rows, devices)
    pieces = jnp.pad(mine.reshape(rows, lanes), ((0, full - rows), (0, 0)))
    pieces = pieces.reshape(devices, full // devices, lanes)
    pieces = lax.all_to_all(pieces, axes, 0, 0, tiled=True)
    spread = pl.pallas_call(
        add_up,
        out_shape=pltpu.VMEM(pieces.shape, F32),
        out_specs=vmem,
        compiler_params=limit(8),
        name="add_up",
    )(pieces)
    half = lax.all_to_all(spread, axes, 0, 0, tiled=True)
    half = half.reshape(full, lanes)[:rows].reshape(2, LANES, lanes)
    rest = lax.ppermute(half, "gy", pair)
    ready, hot, own = pl.pallas_call(
        lambda *refs: begin(order, width, *refs),
        in_specs=(vmem,) * 2,
        out_shape=(
            pltpu.VMEM((2, lanes, padded), BF16),
            pltpu.VMEM((2, LANES, padded), BF16),
            pltpu.VMEM((lanes, 2 * LANES), BF16),
        ),
        out_specs=(vmem,) * 3,
        scratch_shapes=[pltpu.VMEM((8, padded), jnp.int32)],
        compiler_params=limit(8),
        cost_estimate=pl.CostEstimate(flops=2 * 10**9, transcendentals=0, bytes_accessed=8 * 10**6),
        name="begin",
    )(half, held)
    return pl.pallas_call(
        fit,
        out_shape=jax.ShapeDtypeStruct((order, width), F32),
        in_specs=(smem,) + (vmem,) * 6,
        out_specs=pl.BlockSpec(memory_space=pl.ANY),
        scratch_shapes=[
            pltpu.VMEM((lanes, 2 * LANES), BF16),
            pltpu.VMEM((2, lanes, 2 * LANES), BF16),
            pltpu.VMEM((4 * order, snaps), BF16),
            pltpu.VMEM((2, snaps, snaps), BF16),
            pltpu.VMEM((2, 2, lanes, 2 * TILE), BF16),
            pltpu.VMEM((2, 2, lanes, 2 * TILE), BF16),
            pltpu.VMEM((2, 2, lanes, max(padded // TILE % 4, 1) * TILE), BF16),
            pltpu.VMEM((order, padded), F32),
            pltpu.VMEM((order, padded), F32),
            pltpu.VMEM((order, snaps), F32),
            pltpu.VMEM((4, order, LANES), F32),
            pltpu.VMEM((1, padded), F32),
            pltpu.VMEM((2, order, LANES), F32),
            pltpu.VMEM((order, width), F32),
            pltpu.SemaphoreType.DMA((order // 8,)),
        ],
        compiler_params=limit(36),
        name="fit",
    )(core, half, rest, ready, hot, own, weight)


def solution(mesh):
    split_rows = P(("gx", "gy"), None)
    return jax.shard_map(
        on_device,
        mesh=mesh,
        in_specs=(split_rows, split_rows, split_rows, P(), P()),
        out_specs=P(),
        check_vma=False,
    )
```

```python
import math

import jax
import jax.numpy as jnp
from jax import lax
from jax.experimental import pallas as pl
from jax.experimental.pallas import tpu as pltpu
from jax.sharding import PartitionSpec as P

LANES = 128
TILE = 256
GROUP = 7
F32 = jnp.float32
BF16 = jnp.bfloat16
ROWS = ((1,), (0,))


def limit(mebibytes):
    return pltpu.CompilerParams(vmem_limit_bytes=mebibytes * 2**20)


def round_up(value, unit):
    return -(-value // unit) * unit


def dot(a, b, contract=ROWS):
    return lax.dot_general(a, b, (contract, ((), ())), preferred_element_type=F32)


def split(value):
    high = value.astype(BF16)
    return high, (value - high.astype(F32)).astype(BF16)


def project(core_ref, basis_ref, snaps_ref, rates_ref, pairs_ref, mine_ref, other_ref, held_ref, basis_buf, snaps_buf, rates_buf, sems, pair_sem):
    order = basis_ref.shape[0]
    count, size = sems.shape[0], snaps_buf.shape[0] // sems.shape[0]
    copies = []
    for k in range(count):
        here = pl.ds(k * size, size)
        mine = [
            pltpu.make_async_copy(basis_ref.at[:, here], basis_buf.at[:, here], sems.at[k, 0]),
            pltpu.make_async_copy(snaps_ref.at[here, :], snaps_buf.at[here, :], sems.at[k, 1]),
            pltpu.make_async_copy(rates_ref.at[here, :], rates_buf.at[here, :], sems.at[k, 2]),
        ]
        for copy in mine:
            copy.start()
        copies.append(mine)
    hold = pltpu.make_async_copy(pairs_ref, held_ref, pair_sem)
    hold.start()
    total = [0.0, 0.0]
    for k in range(count):
        for copy in copies[k]:
            copy.wait()
        here = slice(k * size, (k + 1) * size)
        basis = basis_buf[:, here]
        total = [t + dot(basis, buf[here, :]) for t, buf in zip(total, (snaps_buf, rates_buf))]
    blank = jnp.zeros((LANES - order, mine_ref.shape[2]), F32)
    first = core_ref[0] == 0
    for k in range(2):
        left, right = jnp.split(total[k], 2, axis=1)
        mine_ref[k, :order, :] = jnp.where(first, left, right)
        other_ref[k, :order, :] = jnp.where(first, right, left)
        mine_ref[k, order:, :] = blank
        other_ref[k, order:, :] = blank
    hold.wait()


def add_up(parts_ref, out_ref):
    devices = parts_ref.shape[0]
    for kind in range(2):
        total = parts_ref[kind]
        for k in range(kind + 2, devices, 2):
            total += parts_ref[k]
        for k in range(kind, devices, 2):
            out_ref[k] = total


def one_hot(index):
    group = 16
    wanted = jnp.broadcast_to(index, (group, index.shape[1])).astype(BF16)
    row = lax.broadcasted_iota(jnp.int32, wanted.shape, 0).astype(F32)
    one, zero = jnp.ones(wanted.shape, BF16), jnp.zeros(wanted.shape, BF16)
    parts = [jnp.where((row + top).astype(BF16) == wanted, one, zero) for top in range(0, LANES, group)]
    return jnp.concatenate(parts, axis=0)


def product(table, hots):
    first, second = (dot(table, jnp.concatenate([hot, hot], axis=0)) for hot in hots)
    return split(first * second)


def make_table(coeffs, order):
    high, low = split(jnp.transpose(coeffs))
    lane = lax.broadcasted_iota(jnp.int32, high.shape, 1)
    high = jnp.where(lane == order, 1.0, high.astype(F32)).astype(BF16)
    return jnp.concatenate([high, low], axis=1)


def begin(order, width, mine_ref, pairs_ref, ready_ref, hot_ref, table_ref, index_ref):
    table_ref[...] = make_table(mine_ref[0], order)
    table = table_ref[...]
    padded = index_ref.shape[1]
    index_ref[0:2, : pairs_ref.shape[1]] = pairs_ref[...]
    turned = pltpu.roll(index_ref[...], order + 1, axis=1)
    row = lax.broadcasted_iota(jnp.int32, turned.shape, 0)
    lane = lax.broadcasted_iota(jnp.int32, turned.shape, 1)
    linear = jnp.where((row == 0) & (lane > 0), lane - 1, order)
    index_ref[...] = jnp.where(lane <= order, linear, jnp.where(lane < width, turned, order + 1))
    for left in range(0, padded, TILE):
        here = slice(left, left + TILE)
        index = index_ref[:, here].astype(F32)
        hots = [one_hot(index[k : k + 1]) for k in range(2)]
        for k in range(2):
            hot_ref[k, :, here] = hots[k]
        ready_ref[0, :, here], ready_ref[1, :, here] = product(table, hots)


def fit(
    core_ref, mine_ref, other_ref, ready_ref, hot_ref, own_ref, weight_ref, out_ref,
    far_ref, table_ref, left_ref, gram_ref, even_ref, odd_ref, rest_ref, b_ref, s_ref, v_ref, acc_ref, extra_ref, mix_ref, x_ref, sems,
):
    order, width = out_ref.shape
    lanes = mine_ref.shape[2]
    snaps = 2 * lanes
    padded = hot_ref.shape[2]
    wide = GROUP * TILE
    groups = padded // (2 * wide) * 2
    spare = padded // TILE - GROUP * groups
    assert groups >= 2
    core = core_ref[0]

    def place(start, size):
        return pl.ds(start if isinstance(start, int) else pl.multiple_of(start, TILE), size)

    def build(data_ref, start, size):
        for left in range(0, size, TILE):
            here = place(start + left, TILE)
            there = slice(left, left + TILE)
            parts = product(far_ref[...], [hot_ref[k, :, here] for k in range(2)])
            for k in range(2):
                data_ref[k, core, :, there] = ready_ref[k, :, here]
                data_ref[k, 1 - core, :, there] = parts[k]

    def load(data_ref, k, left, size):
        return data_ref[k, :, :, left : left + size].reshape(snaps, size)

    def multiply(data_ref, start, size):
        weighted = []
        terms = [0.0] * 4
        for left in range(0, size, TILE):
            here = place(start + left, TILE)
            one = dot(left_ref[...], load(data_ref, 0, left, TILE))
            two = dot(left_ref[0 : 2 * order, :], load(data_ref, 1, left, TILE))
            both = one[: 2 * order] + one[2 * order :] + two
            extra = extra_ref[0:1, here]
            b = both[:order]
            scaled = extra * b
            s = both[order:] + scaled
            b_ref[:, here] = b
            s_ref[:, here] = s
            weighted.append(scaled.astype(BF16))
            square = s * s
            new = (scaled * b, square, extra * square, scaled * s)
            terms = [t + n[:, :LANES] + n[:, LANES:] for t, n in zip(terms, new)]
        v_ref[...] += dot(jnp.concatenate(weighted, axis=1), load(data_ref, 0, 0, size), ((1,), (1,)))
        for k in range(4):
            acc_ref[k] += terms[k]

    def whole(k):
        mine, other = mine_ref[k], other_ref[k]
        return jnp.concatenate([jnp.where(core == 0, mine, other), jnp.where(core == 0, other, mine)], axis=1)

    far_ref[...] = make_table(other_ref[0], order)
    table_ref[core] = own_ref[...]
    table_ref[1 - core] = far_ref[...]
    mean = jnp.sum(weight_ref[...], axis=1, keepdims=True) * (1.0 / width)
    extra_ref[...] = jnp.zeros_like(extra_ref)
    extra_ref[:, :width] = weight_ref[...] - mean
    v_ref[...] = jnp.zeros_like(v_ref)
    acc_ref[...] = jnp.zeros_like(acc_ref)
    build(even_ref, 0, wide)
    if spare:
        build(rest_ref, groups * wide, spare * TILE)
    coeffs = whole(0)
    coeffs_high, coeffs_low = split(coeffs)
    table = table_ref[...].reshape(snaps, 2 * LANES)
    high, low = table[:, :LANES], table[:, LANES:]
    cross = dot(table, jnp.concatenate([coeffs_high, coeffs_high], axis=0)) + dot(high, coeffs_low)
    square_high, square_low = split(coeffs * coeffs)
    turned = high.astype(F32) + low.astype(F32)
    turned_high, turned_low = split(turned * turned)
    squares = dot(
        jnp.concatenate([turned_high, turned_low], axis=1),
        jnp.concatenate([square_high, square_high], axis=0),
    ) + dot(turned_high, square_low)
    gram_high, gram_low = split(1.0 + cross + 0.5 * (cross * cross + squares))
    gram_ref[0] = gram_high
    gram_ref[1] = gram_low

    def times_gram(high, low):
        both = dot(jnp.concatenate([high, low], axis=0), gram_ref[0])
        return both[:order] + both[order:] + dot(high, gram_ref[1])

    rates = whole(1)[:order] * (1.0 / math.sqrt(snaps))
    rates_high, rates_low = split(rates)
    u = times_gram(rates_high, rates_low)
    m0 = jnp.sum(rates * u, axis=1, keepdims=True)
    shift = jnp.sum(u * u, axis=1, keepdims=True) / (snaps * m0)
    along = u * (1.0 / snaps) - shift * rates
    along_high, along_low = split(along)
    left_ref[0:order, :] = rates_high
    left_ref[order : 2 * order, :] = along_high
    left_ref[2 * order : 3 * order, :] = rates_low
    left_ref[3 * order : 4 * order, :] = along_low
    if spare:
        multiply(rest_ref, groups * wide, spare * TILE)

    def body(step, carry):
        first = 2 * step
        build(odd_ref, (first + 1) * wide, wide)
        multiply(even_ref, first * wide, wide)
        build(even_ref, (first + 2) * wide, wide)
        multiply(odd_ref, (first + 1) * wide, wide)
        return carry

    lax.fori_loop(0, groups // 2 - 1, body, 0)
    build(odd_ref, (groups - 1) * wide, wide)
    multiply(even_ref, (groups - 2) * wide, wide)
    multiply(odd_ref, (groups - 1) * wide, wide)

    total = [jnp.sum(acc_ref[k], axis=1, keepdims=True) for k in range(4)]
    bb_extra, ss, ss_extra, bs_extra = total
    ratio = bb_extra / m0
    alpha0 = 1.0 / (shift + mean + ratio)
    perp = ss - ratio * bb_extra
    image = times_gram(along_high, along_low) + v_ref[...] - ratio * u
    energy = (
        jnp.sum(image * image, axis=1, keepdims=True) * (1.0 / snaps)
        + mean * perp
        + ss_extra
        - 2.0 * ratio * bs_extra
        + ratio * ratio * bb_extra
    )
    rr1 = alpha0 * alpha0 * perp
    beta = rr1 / m0
    alpha1 = rr1 / (alpha0 * alpha0 * energy - rr1 * beta / alpha0)
    mix_ref[0] = jnp.broadcast_to(alpha0 + alpha1 * (beta + alpha0 * ratio), (order, LANES))
    mix_ref[1] = jnp.broadcast_to(-alpha1 * alpha0, (order, LANES))

    def copy(group):
        rows = pl.ds(pl.multiple_of(group * 8, 8), 8)
        return pltpu.make_async_copy(x_ref.at[rows, :], out_ref.at[rows, :], sems.at[group])

    def combine(group, carry):
        rows = pl.ds(pl.multiple_of(group * 8, 8), 8)
        on_b = mix_ref[0, rows, :]
        on_s = mix_ref[1, rows, :]
        for left in range(0, width, LANES):
            here = slice(left, min(left + LANES, width))
            size = here.stop - here.start
            x_ref[rows, here] = on_b[:, :size] * b_ref[rows, here] + on_s[:, :size] * s_ref[rows, here]
        copy(group).start()
        return carry

    def finish(group, carry):
        copy(group).wait()
        return carry

    lax.fori_loop(0, order // 8, combine, 0)
    lax.fori_loop(0, order // 8, finish, 0)


def on_device(basis, snapshots, derivatives, quad_pairs, penalty):
    axes = ("gx", "gy")
    devices = lax.axis_size("gx") * lax.axis_size("gy")
    length, order = basis.shape
    snaps = snapshots.shape[1]
    steps = length // TILE if length % TILE == 0 else 1
    count = quad_pairs.shape[1]
    width = 1 + order + count
    padded = round_up(width, TILE)
    assert order + 2 <= LANES and order % 8 == 0 and snaps % (2 * LANES) == 0
    assert lax.axis_size("gy") % 2 == 0
    vmem = pl.BlockSpec(memory_space=pltpu.VMEM)
    smem = pl.BlockSpec(memory_space=pltpu.SMEM)
    lanes = snaps // 2
    core = (lax.axis_index("gy") % 2).reshape(1)
    pair = [(k, k ^ 1) for k in range(lax.axis_size("gy"))]
    mine, other, held = pl.pallas_call(
        project,
        in_specs=(smem,) + (pl.BlockSpec(memory_space=pltpu.HBM),) * 4,
        out_shape=(pltpu.VMEM((2, LANES, lanes), F32),) * 2 + (pltpu.VMEM(quad_pairs.shape, jnp.int32),),
        out_specs=(vmem,) * 3,
        scratch_shapes=[
            pltpu.VMEM((order, length), BF16),
            pltpu.VMEM((length, snaps), BF16),
            pltpu.VMEM((length, snaps), BF16),
            pltpu.SemaphoreType.DMA((steps, 3)),
            pltpu.SemaphoreType.DMA,
        ],
        compiler_params=limit(8),
        name="project",
    )(core, *(pltpu.with_memory_space_constraint(a, pltpu.HBM) for a in (basis.T, snapshots, derivatives, quad_pairs)))
    mine, weight = lax.optimization_barrier((mine + lax.ppermute(other, "gy", pair), penalty.reshape(1, width)))
    rows = 2 * LANES
    full = round_up(rows, devices)
    pieces = jnp.pad(mine.reshape(rows, lanes), ((0, full - rows), (0, 0)))
    pieces = pieces.reshape(devices, full // devices, lanes)
    pieces = lax.all_to_all(pieces, axes, 0, 0, tiled=True)
    spread = pl.pallas_call(
        add_up,
        out_shape=pltpu.VMEM(pieces.shape, F32),
        out_specs=vmem,
        compiler_params=limit(8),
        name="add_up",
    )(pieces)
    half = lax.all_to_all(spread, axes, 0, 0, tiled=True)
    half = half.reshape(full, lanes)[:rows].reshape(2, LANES, lanes)
    rest = lax.ppermute(half, "gy", pair)
    ready, hot, own = pl.pallas_call(
        lambda *refs: begin(order, width, *refs),
        in_specs=(vmem,) * 2,
        out_shape=(
            pltpu.VMEM((2, lanes, padded), BF16),
            pltpu.VMEM((2, LANES, padded), BF16),
            pltpu.VMEM((lanes, 2 * LANES), BF16),
        ),
        out_specs=(vmem,) * 3,
        scratch_shapes=[pltpu.VMEM((8, padded), jnp.int32)],
        compiler_params=limit(8),
        cost_estimate=pl.CostEstimate(flops=2 * 10**9, transcendentals=0, bytes_accessed=8 * 10**6),
        name="begin",
    )(half, held)
    return pl.pallas_call(
        fit,
        out_shape=jax.ShapeDtypeStruct((order, width), F32),
        in_specs=(smem,) + (vmem,) * 6,
        out_specs=pl.BlockSpec(memory_space=pl.ANY),
        scratch_shapes=[
            pltpu.VMEM((lanes, 2 * LANES), BF16),
            pltpu.VMEM((2, lanes, 2 * LANES), BF16),
            pltpu.VMEM((4 * order, snaps), BF16),
            pltpu.VMEM((2, snaps, snaps), BF16),
            pltpu.VMEM((2, 2, lanes, GROUP * TILE), BF16),
            pltpu.VMEM((2, 2, lanes, GROUP * TILE), BF16),
            pltpu.VMEM((2, 2, lanes, max(padded // TILE % (2 * GROUP), 1) * TILE), BF16),
            pltpu.VMEM((order, padded), F32),
            pltpu.VMEM((order, padded), F32),
            pltpu.VMEM((order, snaps), F32),
            pltpu.VMEM((4, order, LANES), F32),
            pltpu.VMEM((1, padded), F32),
            pltpu.VMEM((2, order, LANES), F32),
            pltpu.VMEM((order, width), F32),
            pltpu.SemaphoreType.DMA((order // 8,)),
        ],
        compiler_params=limit(36),
        name="fit",
    )(core, half, rest, ready, hot, own, weight)


def solution(mesh):
    split_rows = P(("gx", "gy"), None)
    return jax.shard_map(
        on_device,
        mesh=mesh,
        in_specs=(split_rows, split_rows, split_rows, P(), P()),
        out_specs=P(),
        check_vma=False,
    )
```
